32 devices in a mesh: dp: 32 (over z, y, x, core).
Axes of the slice: x: 2, y: 2, z: 4, core: 2. Of those that a mesh axis runs over, the one named last changes fastest.
Arguments:
- tokens: bfloat16 [32768, 1024], P('dp'), may hold values from -80 to 80
- seg_ids: int32 [32, 1024], P('dp'), may hold values from 0 to 3, as said below
- counts: int32 [32], replicated, may hold values from 1 to 4, as said below
- positives: int32 [128], P('dp'), may hold values from 0 to 127, as said below
- w_qkv: bfloat16 [1024, 1536], replicated, may hold values from -0.1875 to 0.1875
- w_out: bfloat16 [512, 1024], replicated, may hold values from -0.25 to 0.25
- ln_gain: float32 [1024], replicated, may hold values from 0.1 to 1.9
- w_proj: bfloat16 [1024, 2048], replicated, may hold values from -0.1875 to 0.1875
Outputs:
- loss: float32 [128], P('dp')
- grad_pooled: float32 [128, 1024], P('dp')
The draws below stay inside these ranges and needn't reach their ends.
Inputs may be any that keep to these rules, and one draw needn't show every extreme that they name: `seg_ids`: within a rank, the ids never fall and every id from 0 to 3 occurs. Rank r's live segments are its slots 0 to counts[r] - 1; the other slots hold padding; some rank has all 4 live. `positives`: a live slot of another rank, as rank times 4 plus slot.
All inputs are finite; a program needn't handle non-finite values.
Results may differ from the reference program's by a relative error of at most 0.008.
Values may be sent and summed in bfloat16 or wider, within the bound.
A program may use at most 192 MiB of HBM per device.

```python
import jax
import jax.numpy as jnp
from jax import lax

D = 1024
HEADS = 8
HEAD_DIM = 64
EMBED = 2048
TOK_DEV = 1024
SEG_DEV = 4
TOKENS = 32768
NKEYS = 128
N_DP = 32


def segment_plan(key):
    key = jax.random.fold_in(key, 7)
    key_count, key_full, key_rank, key_pick, key_length = jax.random.split(key, 5)
    counts = jax.random.randint(key_count, (N_DP,), 1, SEG_DEV + 1, dtype=jnp.int32)
    full_rank = jax.random.randint(key_full, (), 0, N_DP, dtype=jnp.int32)
    counts = jnp.where(jnp.arange(N_DP, dtype=jnp.int32) == full_rank, SEG_DEV, counts).astype(jnp.int32)
    owner = jnp.repeat(jnp.arange(N_DP, dtype=jnp.int32), SEG_DEV)
    offset = jax.random.randint(key_rank, (NKEYS,), 1, N_DP, dtype=jnp.int32)
    target_rank = (owner + offset) % N_DP
    picks = jax.random.randint(key_pick, (NKEYS,), 0, 1048576, dtype=jnp.int32)
    target_slot = picks % counts[target_rank]
    positives = (target_rank * SEG_DEV + target_slot).astype(jnp.int32)
    length_weights = jax.random.randint(key_length, (N_DP, SEG_DEV), 1, 3, dtype=jnp.int32)
    cumulative = jnp.cumsum(length_weights, axis=1).astype(jnp.int32)
    total = cumulative[:, -1:]
    ends = (TOK_DEV - SEG_DEV) * cumulative // total
    starts = ends[:, :-1] + jnp.arange(1, SEG_DEV, dtype=jnp.int32)[None, :]
    position = jnp.arange(TOK_DEV, dtype=jnp.int32)
    segment = jnp.sum((position[None, :, None] >= starts[:, None, :]).astype(jnp.int32), axis=2)
    return (counts, positives, segment.astype(jnp.int32))


def draw_tokens(key, part):
    counts, positives, segment = segment_plan(key)
    key_base = jax.random.fold_in(key, 0)
    key_basis = jax.random.fold_in(key, 3)
    values = jnp.clip(jax.random.normal(key_base, (TOKENS, D), jnp.float32), -6.0, 6.0)
    basis = jnp.clip(jax.random.normal(key_basis, (NKEYS, D), jnp.float32), -4.0, 4.0)
    direction = basis + jnp.take(basis, positives, axis=0)
    slot_of = (jnp.arange(N_DP, dtype=jnp.int32)[:, None] * SEG_DEV + segment).reshape(TOKENS)
    values = values + jnp.take(direction, slot_of, axis=0)
    values = jnp.clip(values, -80.0, 80.0)
    return values.astype(jnp.bfloat16)


def draw_seg_ids(key, part):
    return segment_plan(key)[2]


def draw_counts(key, part):
    return segment_plan(key)[0]


def draw_positives(key, part):
    return segment_plan(key)[1]


def gaussian(own_key, shape, spread, limit, kind=jnp.bfloat16):
    drawn = jax.random.normal(own_key, shape, jnp.float32) * spread
    return jnp.minimum(jnp.maximum(drawn, -limit), limit).astype(kind)


def setup_inputs(seed: int = 0) -> dict:
    key_list = jax.random.split(jax.random.key(seed), 9)
    return {
        "tokens": draw_tokens(jax.random.fold_in(key_list[8], 71), 0),
        "seg_ids": draw_seg_ids(jax.random.fold_in(key_list[8], 71), 0),
        "counts": draw_counts(jax.random.fold_in(key_list[8], 71), 0),
        "positives": draw_positives(jax.random.fold_in(key_list[8], 71), 0),
        "w_qkv": gaussian(key_list[4], (D, 3 * HEADS * HEAD_DIM), D ** -0.5, 0.1875),
        "w_out": gaussian(key_list[5], (HEADS * HEAD_DIM, D), (HEADS * HEAD_DIM) ** -0.5, 0.25),
        "ln_gain": jnp.clip(1.0 + 0.18 * jax.random.normal(key_list[6], (D,), jnp.float32), 0.1, 1.9),
        "w_proj": gaussian(key_list[7], (D, EMBED), D ** -0.5, 0.1875),
    }


logit_scale = 20.0

def attend(tok_rows, segment, w_qkv, w_out, ln_gain):
    rows = tok_rows.shape[0]
    width = w_out.shape[0]
    head_dim = width // HEADS
    qkv = jnp.dot(tok_rows, w_qkv, preferred_element_type=jnp.float32).astype(jnp.bfloat16)
    qkv = qkv.reshape(rows, 3, HEADS, head_dim).astype(jnp.float32)
    scores = jnp.einsum('qhd,khd->hqk', qkv[:, 0], qkv[:, 1]) * head_dim ** (-0.5)
    same = segment[:, None] == segment[None, :]
    scores = jnp.where(same[None], scores, -1e+30)
    row_max = lax.optimization_barrier(jnp.max(scores, axis=-1, keepdims=True))
    exp_scores = jnp.exp(scores - row_max)
    probs = (exp_scores / lax.optimization_barrier(jnp.sum(exp_scores, axis=-1, keepdims=True))).astype(jnp.bfloat16)
    context = jnp.einsum('hqk,khd->qhd', probs.astype(jnp.float32), qkv[:, 2])
    context = context.astype(jnp.bfloat16).reshape(rows, width)
    resid = tok_rows.astype(jnp.float32) + jnp.dot(context, w_out, preferred_element_type=jnp.float32)
    centre = resid - lax.optimization_barrier(jnp.mean(resid, axis=-1, keepdims=True))
    variance = lax.optimization_barrier(jnp.mean(centre * centre, axis=-1, keepdims=True))
    return (centre * lax.rsqrt(variance + 1e-05) * ln_gain).astype(jnp.bfloat16)

def pool_rows(hidden, segment, slots):
    member = jnp.arange(slots, dtype=jnp.int32)[:, None] == segment[None, :]
    sums = jnp.dot(member.astype(jnp.bfloat16), hidden, preferred_element_type=jnp.float32)
    sizes = lax.optimization_barrier(jnp.sum(member.astype(jnp.float32), axis=1, keepdims=True))
    return (sums / sizes).astype(jnp.bfloat16)

def embed_rows(pooled, w_proj):
    proj = jnp.dot(pooled, w_proj, preferred_element_type=jnp.float32)
    rnorm = lax.rsqrt(lax.optimization_barrier(jnp.sum(proj * proj, axis=-1, keepdims=True)) + 1e-06)
    return (proj * rnorm, rnorm)

def reference(tokens, seg_ids, counts, positives, w_qkv, w_out, ln_gain, w_proj):
    ranks = tokens.reshape(N_DP, TOK_DEV, D)

    def one_rank(pair):
        hidden = attend(pair[0], pair[1], w_qkv, w_out, ln_gain)
        return pool_rows(hidden, pair[1], SEG_DEV)
    pooled = lax.map(one_rank, (ranks, seg_ids)).reshape(NKEYS, D)
    unit, rnorm = embed_rows(pooled, w_proj)
    emb = unit.astype(jnp.bfloat16)
    logits = logit_scale * jnp.dot(emb, emb.T, preferred_element_type=jnp.float32)
    slot_ids = jnp.arange(NKEYS, dtype=jnp.int32)
    live = slot_ids % SEG_DEV < jnp.repeat(counts, SEG_DEV).astype(jnp.int32)
    allowed = live[None, :] & (slot_ids[None, :] != slot_ids[:, None])
    exp_logits = jnp.where(allowed, jnp.exp(logits), 0.0)
    denominator = lax.optimization_barrier(jnp.sum(exp_logits, axis=-1))
    target = slot_ids[None, :] == positives[:, None]
    picked = lax.optimization_barrier(jnp.sum(jnp.where(target, logits, 0.0), axis=-1))
    loss = jnp.where(live, jnp.log(denominator) - picked, 0.0)
    weights = jnp.where(live[:, None], exp_logits / denominator[:, None] - target.astype(jnp.float32), 0.0)
    weights = weights.astype(jnp.bfloat16)
    d_emb = logit_scale * (jnp.dot(weights, emb, preferred_element_type=jnp.float32) + jnp.dot(weights.T, emb, preferred_element_type=jnp.float32))
    radial = lax.optimization_barrier(jnp.sum(d_emb * unit, axis=-1, keepdims=True))
    d_proj = ((d_emb - radial * unit) * rnorm).astype(jnp.bfloat16)
    grad_pooled = jnp.dot(d_proj, w_proj.T, preferred_element_type=jnp.float32)
    return (loss, grad_pooled)
```

```python
import functools

import jax
import jax.numpy as jnp
from jax import lax
from jax.experimental import pallas as pl
from jax.experimental.pallas import tpu as pltpu
from jax.sharding import PartitionSpec as P

HEADS = 8
LOGIT_SCALE = 20.0
MESH = pl.DeviceIdType.MESH
F32 = jnp.float32
BF16 = jnp.bfloat16
EXT = 128
ONES_ROWS = 16
GROUP = 1024
LOG2E = 1.4426950408889634


def dot(a, b, ca, cb):
    return lax.dot_general(a, b, (((ca,), (cb,)), ((), ())), preferred_element_type=F32)


def attend_kernel(
    block, slots,
    seg_hbm, tok_hbm, wqkv_hbm, wout_hbm,
    tok, wout, ctx_t,
    seg_ref, wqkv, qkv, vt, hot, far, s_buf, sem_tok, sem_w,
):
    rows, width = tok.shape
    inner = wout.shape[0]
    head_dim = inner // HEADS
    blocks = rows // block

    tok_copies = [
        pltpu.make_async_copy(
            tok_hbm.at[pl.ds(i * block, block)], tok.at[pl.ds(i * block, block)], sem_tok.at[i]
        )
        for i in range(blocks)
    ]
    w_copies = [
        pltpu.make_async_copy(
            wqkv_hbm.at[:, pl.ds(j * inner, inner)], wqkv.at[:, pl.ds(j * inner, inner)], sem_w.at[j]
        )
        for j in range(3)
    ]
    o_copy = pltpu.make_async_copy(wout_hbm, wout, sem_w.at[3])
    seg_copy = pltpu.make_async_copy(seg_hbm, seg_ref, sem_w.at[4])
    seg_copy.start()
    tok_copies[0].start()
    w_copies[0].start()
    for c in tok_copies[1:] + w_copies[1:]:
        c.start()
    o_copy.start()

    seg_copy.wait()
    seg = seg_ref[...]
    lane = lax.broadcasted_iota(jnp.int32, (rows, 128), 1)
    seg_col = jnp.transpose(jnp.broadcast_to(seg.astype(F32), (128, rows))).astype(jnp.int32)
    hot[...] = jnp.where(seg_col == lane, 1.0, 0.0).astype(BF16)
    far[...] = jnp.where((lane < slots) & (seg_col != lane), -1e30, 0.0).astype(BF16)
    starts = [
        jnp.sum(jnp.where(seg < s, 1.0, 0.0)).astype(jnp.int32) for s in range(1, slots)
    ]

    for j in range(3):
        w_copies[j].wait()
        cols = slice(j * inner, (j + 1) * inner)
        for i in range(blocks):
            if j == 0:
                tok_copies[i].wait()
            r = slice(i * block, (i + 1) * block)
            part = jnp.dot(tok[r, :], wqkv[:, cols], preferred_element_type=F32).astype(BF16)
            if j == 0:
                qkv[r, cols] = (part.astype(F32) * head_dim ** (-0.5)).astype(BF16)
            elif j == 1:
                qkv[r, cols] = part
            else:
                vt[:, r] = jnp.transpose(part)

    pair_lane = lax.broadcasted_iota(jnp.int32, (block, 128), 1)

    def attend(count, qr, base):
        bounds = [(c, min(c + block, count * 128)) for c in range(0, count * 128, block)]

        def query(h):
            lo = (h * head_dim) // 128 * 128
            own = (pair_lane >= h * head_dim - lo) & (pair_lane < (h + 1) * head_dim - lo)
            q = jnp.where(own, qkv[qr, lo : lo + 128], jnp.zeros((), BF16))
            return jnp.concatenate([q, far[qr, :]], axis=1)

        def score(h, q_ext, c):
            lo = inner + (h * head_dim) // 128 * 128
            a, b = bounds[c]
            kr = pl.ds(pl.multiple_of(base + a, 128), b - a)
            k_ext = jnp.concatenate([qkv[kr, lo : lo + 128], hot[kr, :]], axis=1)
            part = dot(k_ext, q_ext, 1, 1)
            s_buf[h % 2, a:b, :] = part
            return jnp.max(part, axis=0, keepdims=True)

        q_ext = query(0)
        top = functools.reduce(
            jnp.maximum, [score(0, q_ext, c) for c in range(len(bounds))]
        )
        for h in range(HEADS):
            hr = slice(h * head_dim, (h + 1) * head_dim)
            if h + 1 < HEADS:
                q_ext = query(h + 1)
            tops = []
            o = None
            for c, (a, b) in enumerate(bounds):
                if h + 1 < HEADS:
                    tops.append(score(h + 1, q_ext, c))
                p = jnp.exp2((s_buf[h % 2, a:b, :] - top) * LOG2E).astype(BF16)
                kr = pl.ds(pl.multiple_of(base + a, 128), b - a)
                v_ext = jnp.concatenate([vt[hr, kr], jnp.ones((ONES_ROWS, b - a), BF16)], axis=0)
                part = jnp.dot(v_ext, p, preferred_element_type=F32)
                o = part if o is None else o + part
            ctx_t[hr, qr] = (o[:head_dim] / o[head_dim : head_dim + 1]).astype(BF16)
            if tops:
                top = functools.reduce(jnp.maximum, tops)

    def step(i, carry):
        begin = i * block
        lo = jnp.int32(0)
        hi = jnp.int32(rows)
        for s in starts:
            lo = jnp.where(s <= begin, jnp.maximum(lo, s), lo)
            hi = jnp.where(s >= begin + block, jnp.minimum(hi, s), hi)
        first = lo // 128
        count = (hi + 127) // 128 - first
        qr = pl.ds(pl.multiple_of(begin, block), block)
        base = first * 128
        for n in range(block // 128, rows // 128 + 1):

            @pl.when(count == n)
            def _():
                attend(n, qr, base)

        return carry

    lax.fori_loop(0, blocks, step, 0)
    o_copy.wait()


def exchange_kernel(
    n, slots, block,
    counts_ref, pos_ref, seg_ref, gain_ref, tok, wout, ctx_t, wproj_hbm,
    gath, wproj,
    msg_ref, sums, send_sem, recv_sem, fwd_sem, got_sem, own_sem, w_sem,
):
    me = lax.axis_index("dp")
    chips = n // 2
    core = lax.rem(me, 2)
    chip = me // 2
    other = chip * 2 + (1 - core)
    rows, width = tok.shape
    barrier = pltpu.get_barrier_semaphore()

    def peer_of(d):
        return lax.rem(chip + d, chips) * 2 + core

    def greet(d, c):
        pl.semaphore_signal(barrier, inc=1, device_id=(peer_of(d),), device_id_type=MESH)
        return c

    lax.fori_loop(1, chips, greet, 0)
    pl.semaphore_signal(barrier, inc=1, device_id=(other,), device_id_type=MESH)
    w_copy = pltpu.make_async_copy(wproj_hbm, wproj, w_sem)
    w_copy.start()

    total_sum = None
    for i in range(rows // block):
        qr = slice(i * block, (i + 1) * block)
        resid = tok[qr, :].astype(F32) + dot(ctx_t[:, qr], wout[...], 0, 0)
        centre = resid - jnp.mean(resid, axis=-1, keepdims=True)
        variance = jnp.mean(centre * centre, axis=-1, keepdims=True)
        hidden = (centre * lax.rsqrt(variance + 1e-05) * gain_ref[...]).astype(BF16)
        slot = lax.broadcasted_iota(jnp.int32, (8, block), 0)
        member = jnp.where(slot == seg_ref[:, qr], 1.0, 0.0).astype(BF16)
        part = jnp.dot(member, hidden, preferred_element_type=F32)
        if i == 0:
            sums[...] = part
        else:
            sums[...] += part

    slot = lax.broadcasted_iota(jnp.int32, (8, rows), 0)
    sizes = jnp.sum(jnp.where(slot == seg_ref[...], 1.0, 0.0), axis=1, keepdims=True)
    pooled = (sums[...] / jnp.maximum(sizes, 1.0)).astype(BF16)
    msg_ref[:, :width] = pooled[:slots]
    row = lax.broadcasted_iota(jnp.int32, (slots, EXT), 0)
    col = lax.broadcasted_iota(jnp.int32, (slots, EXT), 1)
    ext = jnp.where((col == 2) & (row < counts_ref[me]), 1, 0)
    for s in range(slots):
        p_rank = pos_ref[s] // slots
        p_slot = pos_ref[s] - p_rank * slots
        ext = jnp.where((row == s) & (col == 0), p_rank, ext)
        ext = jnp.where((row == s) & (col == 1), p_slot, ext)
    msg_ref[:, width:] = ext.astype(F32).astype(BF16)

    pl.semaphore_wait(barrier, chips)
    own = pltpu.make_async_copy(msg_ref, gath.at[me], own_sem)
    own.start()

    def send_to(d):
        return pltpu.make_async_remote_copy(
            src_ref=msg_ref, dst_ref=gath.at[me],
            send_sem=send_sem.at[d], recv_sem=recv_sem.at[d],
            device_id=(peer_of(d),), device_id_type=MESH,
        )

    def relay(d):
        src = lax.rem(chip + chips - d, chips) * 2 + core
        return pltpu.make_async_remote_copy(
            src_ref=gath.at[src], dst_ref=gath.at[src],
            send_sem=fwd_sem.at[d], recv_sem=got_sem.at[d],
            device_id=(other,), device_id_type=MESH,
        )

    mine = pltpu.make_async_remote_copy(
        src_ref=msg_ref, dst_ref=gath.at[me],
        send_sem=fwd_sem.at[0], recv_sem=got_sem.at[0],
        device_id=(other,), device_id_type=MESH,
    )

    def send(d, c):
        send_to(d).start()
        return c

    def forward(d, c):
        send_to(d).wait_recv()
        relay(d).start()
        return c

    def arrive(d, c):
        send_to(d).wait_send()
        relay(d).wait()
        return c

    lax.fori_loop(1, chips, send, 0)
    mine.start()
    lax.fori_loop(1, chips, forward, 0)
    own.wait()
    mine.wait()
    lax.fori_loop(1, chips, arrive, 0)
    w_copy.wait()


def loss_kernel(
    n, slots,
    gath, wproj,
    loss_ref, grad_ref,
    allp, unit, scale, wts, wts_t,
):
    me = lax.axis_index("dp")
    total = n * slots
    width = wproj.shape[0]
    per = 8 // slots

    def place(i, c):
        group = [gath[i * per + k].astype(F32) for k in range(per)]
        allp[pl.ds(pl.multiple_of(i * 8, 8), 8), :] = jnp.concatenate(group, axis=0)
        return c

    lax.fori_loop(0, total // 8, place, 0)

    pooled = allp[:, :width].astype(BF16)
    ext = allp[:, width:]
    proj = jnp.dot(pooled, wproj[...], preferred_element_type=F32)
    rnorm = lax.rsqrt(jnp.sum(proj * proj, axis=-1, keepdims=True) + 1e-06)
    unit_all = proj * rnorm
    unit[...] = unit_all
    scale[...] = jnp.broadcast_to(rnorm, scale.shape)
    emb = unit_all.astype(BF16)
    logits = LOGIT_SCALE * dot(emb, emb, 1, 1)

    row = lax.broadcasted_iota(jnp.int32, (total, total), 0)
    col = lax.broadcasted_iota(jnp.int32, (total, total), 1)
    pick = lax.broadcasted_iota(jnp.int32, (8, EXT), 1)
    live_row = dot(jnp.where(pick == 2, 1.0, 0.0).astype(BF16), ext.astype(BF16), 1, 1)[:1]
    live_col = ext[:, 2:3]
    positive = (ext[:, 0:1] * slots + ext[:, 1:2]).astype(jnp.int32)
    allowed = (live_row > 0.5) & (row != col)
    exp_logits = jnp.where(allowed, jnp.exp(logits), 0.0)
    denominator = jnp.sum(exp_logits, axis=-1, keepdims=True)
    target = col == positive
    picked = jnp.sum(jnp.where(target, logits, 0.0), axis=-1, keepdims=True)
    loss = jnp.where(live_col > 0.5, jnp.log(denominator) - picked, 0.0)
    mine = lax.broadcasted_iota(jnp.int32, (total, 128), 0) == (
        me * slots + lax.broadcasted_iota(jnp.int32, (total, 128), 1)
    )
    loss_ref[...] = jnp.sum(jnp.where(mine, loss, 0.0), axis=0)[:slots]
    weights = jnp.where(
        live_col > 0.5, exp_logits / denominator - jnp.where(target, 1.0, 0.0), 0.0
    )
    wts[...] = weights
    wts_t[...] = jnp.transpose(weights)

    base = pl.ds(pl.multiple_of(me // per * 8, 8), 8)
    d_emb = LOGIT_SCALE * (
        jnp.dot(wts[base, :].astype(BF16), emb, preferred_element_type=F32)
        + jnp.dot(wts_t[base, :].astype(BF16), emb, preferred_element_type=F32)
    )
    unit_own = unit[base, :]
    radial = jnp.sum(d_emb * unit_own, axis=-1, keepdims=True)
    d_proj = ((d_emb - radial * unit_own) * scale[base, :][:, :1]).astype(BF16)
    grad = dot(d_proj, wproj[...], 1, 1)
    part = lax.rem(me, per)
    out = grad[:slots]
    for k in range(1, per):
        out = jnp.where(part == k, grad[k * slots : (k + 1) * slots], out)
    grad_ref[...] = out


def body(n, tokens, seg_ids, counts, positives, w_qkv, w_out, ln_gain, w_proj):
    rows, width = tokens.shape
    slots = positives.shape[0]
    inner = w_out.shape[0]
    embed = w_proj.shape[1]
    block = min(256, rows)
    total = n * slots
    vmem = pl.BlockSpec(memory_space=pltpu.VMEM)
    smem = pl.BlockSpec(memory_space=pltpu.SMEM)
    hbm = pl.BlockSpec(memory_space=pltpu.HBM)
    tokens, seg_hbm, w_qkv, w_out, w_proj = (
        pltpu.with_memory_space_constraint(a, pltpu.HBM)
        for a in (tokens, seg_ids, w_qkv, w_out, w_proj)
    )
    tok, wout, ctx_t = pl.pallas_call(
        functools.partial(attend_kernel, block, slots),
        name="attend",
        out_shape=[
            jax.ShapeDtypeStruct((rows, width), BF16),
            jax.ShapeDtypeStruct(w_out.shape, BF16),
            jax.ShapeDtypeStruct((inner, rows), BF16),
        ],
        in_specs=[hbm, hbm, hbm, hbm],
        out_specs=[vmem, vmem, vmem],
        scratch_shapes=[
            pltpu.VMEM((1, rows), jnp.int32),
            pltpu.VMEM(w_qkv.shape, BF16),
            pltpu.VMEM((rows, 2 * inner), BF16),
            pltpu.VMEM((inner, rows), BF16),
            pltpu.VMEM((rows, 128), BF16),
            pltpu.VMEM((rows, 128), BF16),
            pltpu.VMEM((2, rows, block), F32),
            pltpu.SemaphoreType.DMA((rows // block,)),
            pltpu.SemaphoreType.DMA((5,)),
        ],
        compiler_params=pltpu.CompilerParams(vmem_limit_bytes=32 * 1024 * 1024),
    )(seg_hbm, tokens, w_qkv, w_out)
    gath, wproj = pl.pallas_call(
        functools.partial(exchange_kernel, n, slots, block),
        name="exchange",
        out_shape=[
            jax.ShapeDtypeStruct((n, slots, width + EXT), BF16),
            jax.ShapeDtypeStruct(w_proj.shape, BF16),
        ],
        in_specs=[smem, smem, vmem, vmem, vmem, vmem, vmem, hbm],
        out_specs=[vmem, vmem],
        scratch_shapes=[
            pltpu.VMEM((slots, width + EXT), BF16),
            pltpu.VMEM((8, width), F32),
            pltpu.SemaphoreType.DMA((n // 2,)),
            pltpu.SemaphoreType.DMA((n // 2,)),
            pltpu.SemaphoreType.DMA((n // 2,)),
            pltpu.SemaphoreType.DMA((n // 2,)),
            pltpu.SemaphoreType.DMA,
            pltpu.SemaphoreType.DMA,
        ],
        compiler_params=pltpu.CompilerParams(
            collective_id=0, has_side_effects=True, vmem_limit_bytes=24 * 1024 * 1024
        ),
    )(counts, positives, seg_ids, ln_gain.reshape(1, width), tok, wout, ctx_t, w_proj)
    loss, grad = pl.pallas_call(
        functools.partial(loss_kernel, n, slots),
        name="contrast",
        out_shape=[
            jax.ShapeDtypeStruct((slots,), F32),
            jax.ShapeDtypeStruct((slots, width), F32),
        ],
        in_specs=[vmem, vmem],
        out_specs=[vmem, vmem],
        scratch_shapes=[
            pltpu.VMEM((total, width + EXT), F32),
            pltpu.VMEM((total, embed), F32),
            pltpu.VMEM((total, 128), F32),
            pltpu.VMEM((total, total), F32),
            pltpu.VMEM((total, total), F32),
        ],
        compiler_params=pltpu.CompilerParams(
            vmem_limit_bytes=(24 if total <= 128 else 56) * 1024 * 1024
        ),
    )(gath, wproj)
    return loss, grad


def solution(mesh):
    return jax.shard_map(
        functools.partial(body, mesh.shape["dp"]),
        mesh=mesh,
        in_specs=(P("dp", None), P("dp", None), P(), P("dp"), P(), P(), P(), P()),
        out_specs=(P("dp"), P("dp", None)),
        check_vma=False,
    )
```

```python
import functools

import jax
import jax.numpy as jnp
from jax import lax
from jax.experimental import pallas as pl
from jax.experimental.pallas import tpu as pltpu
from jax.sharding import PartitionSpec as P

HEADS = 8
LOGIT_SCALE = 20.0
MESH = pl.DeviceIdType.MESH
F32 = jnp.float32
BF16 = jnp.bfloat16
EXT = 128
ONES_ROWS = 16
FINISH = 1024
LOG2E = 1.4426950408889634


def dot(a, b, ca, cb):
    return lax.dot_general(a, b, (((ca,), (cb,)), ((), ())), preferred_element_type=F32)


def attend_kernel(
    block, slots,
    seg_hbm, tok_hbm, wqkv_hbm, wout_hbm,
    tok, wout, ctx_t,
    seg_ref, wqkv, qt, kd, vt, hot, far, s_buf, sem_tok, sem_w,
):
    rows, width = tok.shape
    inner = wout.shape[0]
    head_dim = inner // HEADS
    blocks = rows // block

    tok_copies = [
        pltpu.make_async_copy(
            tok_hbm.at[pl.ds(i * block, block)], tok.at[pl.ds(i * block, block)], sem_tok.at[i]
        )
        for i in range(blocks)
    ]
    w_copies = [
        pltpu.make_async_copy(
            wqkv_hbm.at[:, pl.ds(j * inner, inner)], wqkv.at[:, pl.ds(j * inner, inner)], sem_w.at[j]
        )
        for j in range(3)
    ]
    o_copy = pltpu.make_async_copy(wout_hbm, wout, sem_w.at[3])
    seg_copy = pltpu.make_async_copy(seg_hbm, seg_ref, sem_w.at[4])
    seg_copy.start()
    tok_copies[0].start()
    w_copies[1].start()
    for c in tok_copies[1:] + [w_copies[0], w_copies[2]]:
        c.start()
    o_copy.start()

    seg_copy.wait()
    seg = seg_ref[...]
    slot = lax.broadcasted_iota(jnp.int32, (128, rows), 0)
    hot[...] = jnp.transpose(jnp.where(slot == seg, 1.0, 0.0).astype(BF16))
    far[...] = jnp.where((slot < slots) & (slot != seg), -1e30, 0.0).astype(BF16)
    starts = [
        jnp.sum(jnp.where(seg < s, 1.0, 0.0)).astype(jnp.int32) for s in range(1, slots)
    ]

    for j in (1, 0, 2):
        w_copies[j].wait()
        cols = slice(j * inner, (j + 1) * inner)
        tall = block if j == 1 else min(2 * block, rows)
        for i in range(rows // tall):
            if j == 1:
                tok_copies[i].wait()
            r = slice(i * tall, (i + 1) * tall)
            part = jnp.dot(tok[r, :], wqkv[:, cols], preferred_element_type=F32).astype(BF16)
            if j == 0:
                q = (part.astype(F32) * head_dim ** (-0.5)).astype(BF16)
                qt[:, r] = jnp.transpose(q)
            elif j == 1:
                kd[r, :] = part
            else:
                vt[:, r] = jnp.transpose(part)

    def attend(count, qr, base):
        bounds = [(c, min(c + block, count * 128)) for c in range(0, count * 128, block)]

        def query(h):
            hr = slice(h * head_dim, (h + 1) * head_dim)
            lo = h * head_dim % 128
            parts = [qt[hr, qr], far[:, qr]]
            if lo:
                parts.insert(0, jnp.zeros((lo, block), BF16))
            if lo + head_dim < 128:
                parts.insert(-1, jnp.zeros((128 - lo - head_dim, block), BF16))
            return jnp.concatenate(parts, axis=0)

        def score(h, q_ext, c):
            a, b = bounds[c]
            kr = pl.ds(pl.multiple_of(base + a, 128), b - a)
            lo = h * head_dim // 128 * 128
            k_ext = jnp.concatenate([kd[kr, lo : lo + 128], hot[kr, :]], axis=1)
            part = jnp.dot(k_ext, q_ext, preferred_element_type=F32)
            s_buf[h % 2, a:b, :] = part
            return jnp.max(part, axis=0, keepdims=True)

        q_ext = query(0)
        top = functools.reduce(
            jnp.maximum, [score(0, q_ext, c) for c in range(len(bounds))]
        )
        for h in range(HEADS):
            hr = slice(h * head_dim, (h + 1) * head_dim)
            if h + 1 < HEADS:
                q_ext = query(h + 1)
            tops = []
            o = None
            for c, (a, b) in enumerate(bounds):
                if h + 1 < HEADS:
                    tops.append(score(h + 1, q_ext, c))
                p = jnp.exp2((s_buf[h % 2, a:b, :] - top) * LOG2E).astype(BF16)
                kr = pl.ds(pl.multiple_of(base + a, 128), b - a)
                v_ext = jnp.concatenate([vt[hr, kr], jnp.ones((ONES_ROWS, b - a), BF16)], axis=0)
                part = jnp.dot(v_ext, p, preferred_element_type=F32)
                o = part if o is None else o + part
            ctx_t[hr, qr] = (o[:head_dim] / o[head_dim : head_dim + 1]).astype(BF16)
            if tops:
                top = functools.reduce(jnp.maximum, tops)

    def step(i, carry):
        begin = i * block
        lo = jnp.int32(0)
        hi = jnp.int32(rows)
        for s in starts:
            lo = jnp.where(s <= begin, jnp.maximum(lo, s), lo)
            hi = jnp.where(s >= begin + block, jnp.minimum(hi, s), hi)
        first = lo // 128
        count = (hi + 127) // 128 - first
        qr = pl.ds(pl.multiple_of(begin, block), block)
        base = first * 128
        for n in range(block // 128, rows // 128 + 1):

            @pl.when(count == n)
            def _():
                attend(n, qr, base)

        return carry

    lax.fori_loop(0, blocks, step, 0)
    o_copy.wait()


def exchange_kernel(
    n, slots,
    counts_ref, pos_ref, seg_ref, gain_ref, tok, wout, ctx_t, wproj_hbm,
    gath, wproj,
    msg_ref, sums, send_sem, recv_sem, fwd_sem, got_sem, own_sem, w_sem,
):
    me = lax.axis_index("dp")
    chips = n // 2
    core = lax.rem(me, 2)
    chip = me // 2
    other = chip * 2 + (1 - core)
    rows, width = tok.shape
    barrier = pltpu.get_barrier_semaphore()

    def peer_of(d):
        return lax.rem(chip + d, chips) * 2 + core

    def greet(d, c):
        pl.semaphore_signal(barrier, inc=1, device_id=(peer_of(d),), device_id_type=MESH)
        return c

    lax.fori_loop(1, chips, greet, 0)
    pl.semaphore_signal(barrier, inc=1, device_id=(other,), device_id_type=MESH)
    w_copy = pltpu.make_async_copy(wproj_hbm, wproj, w_sem)
    w_copy.start()

    block = min(FINISH, rows)
    for i in range(rows // block):
        qr = slice(i * block, (i + 1) * block)
        resid = tok[qr, :].astype(F32) + dot(ctx_t[:, qr], wout[...], 0, 0)
        centre = resid - jnp.mean(resid, axis=-1, keepdims=True)
        variance = jnp.mean(centre * centre, axis=-1, keepdims=True)
        hidden = (centre * lax.rsqrt(variance + 1e-05) * gain_ref[...]).astype(BF16)
        slot = lax.broadcasted_iota(jnp.int32, (8, block), 0)
        member = jnp.where(slot == seg_ref[:, qr], 1.0, 0.0).astype(BF16)
        part = jnp.dot(member, hidden, preferred_element_type=F32)
        if i == 0:
            sums[...] = part
        else:
            sums[...] += part

    slot = lax.broadcasted_iota(jnp.int32, (8, rows), 0)
    sizes = jnp.sum(jnp.where(slot == seg_ref[...], 1.0, 0.0), axis=1, keepdims=True)
    pooled = (sums[...] / jnp.maximum(sizes, 1.0)).astype(BF16)
    msg_ref[:, :width] = pooled[:slots]
    row = lax.broadcasted_iota(jnp.int32, (slots, EXT), 0)
    col = lax.broadcasted_iota(jnp.int32, (slots, EXT), 1)
    ext = jnp.where((col == 2) & (row < counts_ref[me]), 1, 0)
    for s in range(slots):
        p_rank = pos_ref[s] // slots
        p_slot = pos_ref[s] - p_rank * slots
        ext = jnp.where((row == s) & (col == 0), p_rank, ext)
        ext = jnp.where((row == s) & (col == 1), p_slot, ext)
    msg_ref[:, width:] = ext.astype(F32).astype(BF16)

    pl.semaphore_wait(barrier, chips)
    own = pltpu.make_async_copy(msg_ref, gath.at[me], own_sem)
    own.start()

    def send_to(d):
        return pltpu.make_async_remote_copy(
            src_ref=msg_ref, dst_ref=gath.at[me],
            send_sem=send_sem.at[d], recv_sem=recv_sem.at[d],
            device_id=(peer_of(d),), device_id_type=MESH,
        )

    def relay(d):
        src = lax.rem(chip + chips - d, chips) * 2 + core
        return pltpu.make_async_remote_copy(
            src_ref=gath.at[src], dst_ref=gath.at[src],
            send_sem=fwd_sem.at[d], recv_sem=got_sem.at[d],
            device_id=(other,), device_id_type=MESH,
        )

    mine = pltpu.make_async_remote_copy(
        src_ref=msg_ref, dst_ref=gath.at[me],
        send_sem=fwd_sem.at[0], recv_sem=got_sem.at[0],
        device_id=(other,), device_id_type=MESH,
    )

    def send(d, c):
        send_to(d).start()
        return c

    def forward(d, c):
        send_to(d).wait_recv()
        relay(d).start()
        return c

    def arrive(d, c):
        send_to(d).wait_send()
        relay(d).wait()
        return c

    lax.fori_loop(1, chips, send, 0)
    mine.start()
    lax.fori_loop(1, chips, forward, 0)
    own.wait()
    mine.wait()
    lax.fori_loop(1, chips, arrive, 0)
    w_copy.wait()


def loss_kernel(
    n, slots,
    gath, wproj,
    loss_ref, grad_ref,
    allp, unit, scale, wts, wts_t,
):
    me = lax.axis_index("dp")
    total = n * slots
    width = wproj.shape[0]
    per = 8 // slots

    def place(i, c):
        group = [gath[i * per + k].astype(F32) for k in range(per)]
        allp[pl.ds(pl.multiple_of(i * 8, 8), 8), :] = jnp.concatenate(group, axis=0)
        return c

    lax.fori_loop(0, total // 8, place, 0)

    pooled = allp[:, :width].astype(BF16)
    ext = allp[:, width:]
    proj = jnp.dot(pooled, wproj[...], preferred_element_type=F32)
    rnorm = lax.rsqrt(jnp.sum(proj * proj, axis=-1, keepdims=True) + 1e-06)
    unit_all = proj * rnorm
    unit[...] = unit_all
    scale[...] = jnp.broadcast_to(rnorm, scale.shape)
    emb = unit_all.astype(BF16)
    logits = LOGIT_SCALE * dot(emb, emb, 1, 1)

    row = lax.broadcasted_iota(jnp.int32, (total, total), 0)
    col = lax.broadcasted_iota(jnp.int32, (total, total), 1)
    pick = lax.broadcasted_iota(jnp.int32, (8, EXT), 1)
    live_row = dot(jnp.where(pick == 2, 1.0, 0.0).astype(BF16), ext.astype(BF16), 1, 1)[:1]
    live_col = ext[:, 2:3]
    positive = (ext[:, 0:1] * slots + ext[:, 1:2]).astype(jnp.int32)
    allowed = (live_row > 0.5) & (row != col)
    exp_logits = jnp.where(allowed, jnp.exp(logits), 0.0)
    denominator = jnp.sum(exp_logits, axis=-1, keepdims=True)
    target = col == positive
    picked = jnp.sum(jnp.where(target, logits, 0.0), axis=-1, keepdims=True)
    loss = jnp.where(live_col > 0.5, jnp.log(denominator) - picked, 0.0)
    mine = lax.broadcasted_iota(jnp.int32, (total, 128), 0) == (
        me * slots + lax.broadcasted_iota(jnp.int32, (total, 128), 1)
    )
    loss_ref[...] = jnp.sum(jnp.where(mine, loss, 0.0), axis=0)[:slots]
    weights = jnp.where(
        live_col > 0.5, exp_logits / denominator - jnp.where(target, 1.0, 0.0), 0.0
    )
    wts[...] = weights
    wts_t[...] = jnp.transpose(weights)

    base = pl.ds(pl.multiple_of(me // per * 8, 8), 8)
    both = jnp.concatenate([wts[base, :], wts_t[base, :]], axis=0).astype(BF16)
    parts = jnp.dot(both, emb, preferred_element_type=F32)
    d_emb = LOGIT_SCALE * (parts[:8] + parts[8:])
    unit_own = unit[base, :]
    radial = jnp.sum(d_emb * unit_own, axis=-1, keepdims=True)
    d_proj = ((d_emb - radial * unit_own) * scale[base, :][:, :1]).astype(BF16)
    grad = dot(d_proj, wproj[...], 1, 1)
    part = lax.rem(me, per)
    out = grad[:slots]
    for k in range(1, per):
        out = jnp.where(part == k, grad[k * slots : (k + 1) * slots], out)
    grad_ref[...] = out


def body(n, tokens, seg_ids, counts, positives, w_qkv, w_out, ln_gain, w_proj):
    rows, width = tokens.shape
    slots = positives.shape[0]
    inner = w_out.shape[0]
    embed = w_proj.shape[1]
    block = min(256, rows)
    total = n * slots
    vmem = pl.BlockSpec(memory_space=pltpu.VMEM)
    smem = pl.BlockSpec(memory_space=pltpu.SMEM)
    hbm = pl.BlockSpec(memory_space=pltpu.HBM)
    tokens, seg_hbm, w_qkv, w_out, w_proj = (
        pltpu.with_memory_space_constraint(a, pltpu.HBM)
        for a in (tokens, seg_ids, w_qkv, w_out, w_proj)
    )
    tok, wout, ctx_t = pl.pallas_call(
        functools.partial(attend_kernel, block, slots),
        name="attend",
        out_shape=[
            jax.ShapeDtypeStruct((rows, width), BF16),
            jax.ShapeDtypeStruct(w_out.shape, BF16),
            jax.ShapeDtypeStruct((inner, rows), BF16),
        ],
        in_specs=[hbm, hbm, hbm, hbm],
        out_specs=[vmem, vmem, vmem],
        scratch_shapes=[
            pltpu.VMEM((1, rows), jnp.int32),
            pltpu.VMEM(w_qkv.shape, BF16),
            pltpu.VMEM((inner, rows), BF16),
            pltpu.VMEM((rows, inner), BF16),
            pltpu.VMEM((inner, rows), BF16),
            pltpu.VMEM((rows, 128), BF16),
            pltpu.VMEM((128, rows), BF16),
            pltpu.VMEM((2, rows, block), F32),
            pltpu.SemaphoreType.DMA((rows // block,)),
            pltpu.SemaphoreType.DMA((5,)),
        ],
        compiler_params=pltpu.CompilerParams(vmem_limit_bytes=32 * 1024 * 1024),
    )(seg_hbm, tokens, w_qkv, w_out)
    gath, wproj = pl.pallas_call(
        functools.partial(exchange_kernel, n, slots),
        name="exchange",
        out_shape=[
            jax.ShapeDtypeStruct((n, slots, width + EXT), BF16),
            jax.ShapeDtypeStruct(w_proj.shape, BF16),
        ],
        in_specs=[smem, smem, vmem, vmem, vmem, vmem, vmem, hbm],
        out_specs=[vmem, vmem],
        scratch_shapes=[
            pltpu.VMEM((slots, width + EXT), BF16),
            pltpu.VMEM((8, width), F32),
            pltpu.SemaphoreType.DMA((n // 2,)),
            pltpu.SemaphoreType.DMA((n // 2,)),
            pltpu.SemaphoreType.DMA((n // 2,)),
            pltpu.SemaphoreType.DMA((n // 2,)),
            pltpu.SemaphoreType.DMA,
            pltpu.SemaphoreType.DMA,
        ],
        compiler_params=pltpu.CompilerParams(
            collective_id=0, has_side_effects=True, vmem_limit_bytes=24 * 1024 * 1024
        ),
    )(counts, positives, seg_ids, ln_gain.reshape(1, width), tok, wout, ctx_t, w_proj)
    loss, grad = pl.pallas_call(
        functools.partial(loss_kernel, n, slots),
        name="contrast",
        out_shape=[
            jax.ShapeDtypeStruct((slots,), F32),
            jax.ShapeDtypeStruct((slots, width), F32),
        ],
        in_specs=[vmem, vmem],
        out_specs=[vmem, vmem],
        scratch_shapes=[
            pltpu.VMEM((total, width + EXT), F32),
            pltpu.VMEM((total, embed), F32),
            pltpu.VMEM((total, 128), F32),
            pltpu.VMEM((total, total), F32),
            pltpu.VMEM((total, total), F32),
        ],
        compiler_params=pltpu.CompilerParams(
            vmem_limit_bytes=(24 if total <= 128 else 56) * 1024 * 1024
        ),
    )(gath, wproj)
    return loss, grad


def solution(mesh):
    return jax.shard_map(
        functools.partial(body, mesh.shape["dp"]),
        mesh=mesh,
        in_specs=(P("dp", None), P("dp", None), P(), P("dp"), P(), P(), P(), P()),
        out_specs=(P("dp"), P("dp", None)),
        check_vma=False,
    )
```

```python
import functools

import jax
import jax.numpy as jnp
from jax import lax
from jax.experimental import pallas as pl
from jax.experimental.pallas import tpu as pltpu
from jax.sharding import PartitionSpec as P

HEADS = 8
LOGIT_SCALE = 20.0
MESH = pl.DeviceIdType.MESH
F32 = jnp.float32
BF16 = jnp.bfloat16
EXT = 128
ONES_ROWS = 16
FINISH = 1024
LOG2E = 1.4426950408889634


def dot(a, b, ca, cb):
    return lax.dot_general(a, b, (((ca,), (cb,)), ((), ())), preferred_element_type=F32)


def attend_kernel(
    block, slots,
    seg_hbm, tok_hbm, wqkv_hbm, wout_hbm,
    tok, wout, ctx_t,
    seg_ref, wqkv, qt, kd, vt, hot, far, s_buf, sem_tok, sem_w,
):
    rows, width = tok.shape
    inner = wout.shape[0]
    head_dim = inner // HEADS
    blocks = rows // block

    tok_copies = [
        pltpu.make_async_copy(
            tok_hbm.at[pl.ds(i * block, block)], tok.at[pl.ds(i * block, block)], sem_tok.at[i]
        )
        for i in range(blocks)
    ]
    w_copies = [
        pltpu.make_async_copy(
            wqkv_hbm.at[:, pl.ds(j * inner, inner)], wqkv.at[:, pl.ds(j * inner, inner)], sem_w.at[j]
        )
        for j in range(3)
    ]
    o_copy = pltpu.make_async_copy(wout_hbm, wout, sem_w.at[3])
    seg_copy = pltpu.make_async_copy(seg_hbm, seg_ref, sem_w.at[4])
    seg_copy.start()
    tok_copies[0].start()
    w_copies[1].start()
    for c in tok_copies[1:] + [w_copies[0], w_copies[2]]:
        c.start()
    o_copy.start()

    seg_copy.wait()
    seg = seg_ref[...]
    slot = lax.broadcasted_iota(jnp.int32, (128, rows), 0)
    hot[...] = jnp.transpose(jnp.where(slot == seg, 1.0, 0.0).astype(BF16))
    far[...] = jnp.where((slot < slots) & (slot != seg), -1e30, 0.0).astype(BF16)
    starts = [
        jnp.sum(jnp.where(seg < s, 1.0, 0.0)).astype(jnp.int32) for s in range(1, slots)
    ]

    for j in (1, 0, 2):
        w_copies[j].wait()
        cols = slice(j * inner, (j + 1) * inner)
        tall = block if j == 1 else min(2 * block, rows)
        for i in range(rows // tall):
            if j == 1:
                tok_copies[i].wait()
            r = slice(i * tall, (i + 1) * tall)
            part = jnp.dot(tok[r, :], wqkv[:, cols], preferred_element_type=F32).astype(BF16)
            if j == 0:
                q = (part.astype(F32) * head_dim ** (-0.5)).astype(BF16)
                qt[:, r] = jnp.transpose(q)
            elif j == 1:
                kd[r, :] = part
            else:
                vt[:, r] = jnp.transpose(part)

    def attend(count, qr, base):
        bounds = [(c, min(c + block, count * 128)) for c in range(0, count * 128, block)]

        def query(h):
            hr = slice(h * head_dim, (h + 1) * head_dim)
            lo = h * head_dim % 128
            parts = [qt[hr, qr], far[:, qr]]
            if lo:
                parts.insert(0, jnp.zeros((lo, block), BF16))
            if lo + head_dim < 128:
                parts.insert(-1, jnp.zeros((128 - lo - head_dim, block), BF16))
            return jnp.concatenate(parts, axis=0)

        def score(h, q_ext, c):
            a, b = bounds[c]
            kr = pl.ds(pl.multiple_of(base + a, 128), b - a)
            lo = h * head_dim // 128 * 128
            k_ext = jnp.concatenate([kd[kr, lo : lo + 128], hot[kr, :]], axis=1)
            part = jnp.dot(k_ext, q_ext, preferred_element_type=F32)
            s_buf[h % 2, a:b, :] = part
            return jnp.max(part, axis=0, keepdims=True)

        q_ext = query(0)
        top = functools.reduce(
            jnp.maximum, [score(0, q_ext, c) for c in range(len(bounds))]
        )
        for h in range(HEADS):
            hr = slice(h * head_dim, (h + 1) * head_dim)
            if h + 1 < HEADS:
                q_ext = query(h + 1)
            tops = []
            o = None
            for c, (a, b) in enumerate(bounds):
                if h + 1 < HEADS:
                    tops.append(score(h + 1, q_ext, c))
                p = jnp.exp2((s_buf[h % 2, a:b, :] - top) * LOG2E).astype(BF16)
                kr = pl.ds(pl.multiple_of(base + a, 128), b - a)
                v_ext = jnp.concatenate([vt[hr, kr], jnp.ones((ONES_ROWS, b - a), BF16)], axis=0)
                part = jnp.dot(v_ext, p, preferred_element_type=F32)
                o = part if o is None else o + part
            ctx_t[hr, qr] = (o[:head_dim] / o[head_dim : head_dim + 1]).astype(BF16)
            if tops:
                top = functools.reduce(jnp.maximum, tops)

    def step(i, carry):
        begin = i * block
        lo = jnp.int32(0)
        hi = jnp.int32(rows)
        for s in starts:
            lo = jnp.where(s <= begin, jnp.maximum(lo, s), lo)
            hi = jnp.where(s >= begin + block, jnp.minimum(hi, s), hi)
        first = lo // 128
        count = (hi + 127) // 128 - first
        qr = pl.ds(pl.multiple_of(begin, block), block)
        most = rows // 128
        sizes = sorted({min(n, most) for n in (2, 3, 4, 5, 6)} | {most})
        below = 0
        for n in sizes:

            @pl.when((count > below) & (count <= n))
            def _():
                attend(n, qr, jnp.minimum(first, most - n) * 128)

            below = n

        return carry

    lax.fori_loop(0, blocks, step, 0)
    o_copy.wait()


def each(first, last, f):
    if last - first <= 16:
        for m in range(first, last):
            f(m)
        return

    def one(m, c):
        f(m)
        return c

    lax.fori_loop(first, last, one, 0)


def exchange_kernel(
    n, slots,
    counts_ref, pos_ref, seg_ref, gain_ref, tok, wout, ctx_t, wproj_hbm,
    gath, wproj,
    msg_ref, sums, send_sem, recv_sem, fwd_sem, got_sem, own_sem, w_sem,
):
    me = lax.axis_index("dp")
    chips = n // 2
    core = lax.rem(me, 2)
    chip = me // 2
    other = chip * 2 + (1 - core)
    rows, width = tok.shape
    barrier = pltpu.get_barrier_semaphore()

    def peer_of(d):
        ahead = chip + d
        return jnp.where(ahead < chips, ahead, ahead - chips) * 2 + core

    def greet(d):
        pl.semaphore_signal(barrier, inc=1, device_id=(peer_of(d),), device_id_type=MESH)

    each(1, chips, greet)
    pl.semaphore_signal(barrier, inc=1, device_id=(other,), device_id_type=MESH)
    w_copy = pltpu.make_async_copy(wproj_hbm, wproj, w_sem)
    w_copy.start()

    block = min(FINISH, rows)
    for i in range(rows // block):
        qr = slice(i * block, (i + 1) * block)
        resid = tok[qr, :].astype(F32) + dot(ctx_t[:, qr], wout[...], 0, 0)
        centre = resid - jnp.mean(resid, axis=-1, keepdims=True)
        variance = jnp.mean(centre * centre, axis=-1, keepdims=True)
        hidden = (centre * lax.rsqrt(variance + 1e-05) * gain_ref[...]).astype(BF16)
        slot = lax.broadcasted_iota(jnp.int32, (8, block), 0)
        member = jnp.where(slot == seg_ref[:, qr], 1.0, 0.0).astype(BF16)
        part = jnp.dot(member, hidden, preferred_element_type=F32)
        if i == 0:
            sums[...] = part
        else:
            sums[...] += part

    slot = lax.broadcasted_iota(jnp.int32, (8, rows), 0)
    sizes = jnp.sum(jnp.where(slot == seg_ref[...], 1.0, 0.0), axis=1, keepdims=True)
    pooled = (sums[...] / jnp.maximum(sizes, 1.0)).astype(BF16)
    msg_ref[:, :width] = pooled[:slots]
    row = lax.broadcasted_iota(jnp.int32, (slots, EXT), 0)
    col = lax.broadcasted_iota(jnp.int32, (slots, EXT), 1)
    ext = jnp.where((col == 2) & (row < counts_ref[me]), 1, 0)
    for s in range(slots):
        p_rank = pos_ref[s] // slots
        p_slot = pos_ref[s] - p_rank * slots
        ext = jnp.where((row == s) & (col == 0), p_rank, ext)
        ext = jnp.where((row == s) & (col == 1), p_slot, ext)
    msg_ref[:, width:] = ext.astype(F32).astype(BF16)

    pl.semaphore_wait(barrier, chips)
    own = pltpu.make_async_copy(msg_ref, gath.at[me], own_sem)
    own.start()

    def send_to(d):
        return pltpu.make_async_remote_copy(
            src_ref=msg_ref, dst_ref=gath.at[me],
            send_sem=send_sem.at[d], recv_sem=recv_sem.at[d],
            device_id=(peer_of(d),), device_id_type=MESH,
        )

    def relay(d):
        back = chip - d
        src = jnp.where(back < 0, back + chips, back) * 2 + core
        return pltpu.make_async_remote_copy(
            src_ref=gath.at[src], dst_ref=gath.at[src],
            send_sem=fwd_sem.at[d], recv_sem=got_sem.at[d],
            device_id=(other,), device_id_type=MESH,
        )

    mine = pltpu.make_async_remote_copy(
        src_ref=msg_ref, dst_ref=gath.at[me],
        send_sem=fwd_sem.at[0], recv_sem=got_sem.at[0],
        device_id=(other,), device_id_type=MESH,
    )

    def forward(d):
        send_to(d).wait_recv()
        relay(d).start()

    def arrive(d):
        send_to(d).wait_send()
        relay(d).wait()

    each(1, chips, lambda d: send_to(d).start())
    mine.start()
    each(1, chips, forward)
    own.wait()
    mine.wait()
    each(1, chips, arrive)
    w_copy.wait()


def loss_kernel(
    n, slots,
    gath, wproj,
    loss_ref, grad_ref,
    allp, unit, scale, wts, wts_t,
):
    me = lax.axis_index("dp")
    total = n * slots
    width = wproj.shape[0]
    per = 8 // slots

    def place(i):
        group = [gath[i * per + k].astype(F32) for k in range(per)]
        allp[pl.ds(pl.multiple_of(i * 8, 8), 8), :] = jnp.concatenate(group, axis=0)

    each(0, total // 8, place)

    pooled = allp[:, :width].astype(BF16)
    ext = allp[:, width:]
    proj = jnp.dot(pooled, wproj[...], preferred_element_type=F32)
    rnorm = lax.rsqrt(jnp.sum(proj * proj, axis=-1, keepdims=True) + 1e-06)
    unit_all = proj * rnorm
    unit[...] = unit_all
    scale[...] = jnp.broadcast_to(rnorm, scale.shape)
    emb = unit_all.astype(BF16)
    logits = LOGIT_SCALE * dot(emb, emb, 1, 1)

    row = lax.broadcasted_iota(jnp.int32, (total, total), 0)
    col = lax.broadcasted_iota(jnp.int32, (total, total), 1)
    pick = lax.broadcasted_iota(jnp.int32, (8, EXT), 1)
    live_row = dot(jnp.where(pick == 2, 1.0, 0.0).astype(BF16), ext.astype(BF16), 1, 1)[:1]
    live_col = ext[:, 2:3]
    positive = (ext[:, 0:1] * slots + ext[:, 1:2]).astype(jnp.int32)
    allowed = (live_row > 0.5) & (row != col)
    exp_logits = jnp.where(allowed, jnp.exp(logits), 0.0)
    denominator = jnp.sum(exp_logits, axis=-1, keepdims=True)
    target = col == positive
    picked = jnp.sum(jnp.where(target, logits, 0.0), axis=-1, keepdims=True)
    loss = jnp.where(live_col > 0.5, jnp.log(denominator) - picked, 0.0)
    mine = lax.broadcasted_iota(jnp.int32, (total, 128), 0) == (
        me * slots + lax.broadcasted_iota(jnp.int32, (total, 128), 1)
    )
    loss_ref[...] = jnp.sum(jnp.where(mine, loss, 0.0), axis=0)[:slots]
    weights = jnp.where(
        live_col > 0.5, exp_logits / denominator - jnp.where(target, 1.0, 0.0), 0.0
    )
    wts[...] = weights
    wts_t[...] = jnp.transpose(weights)

    base = pl.ds(pl.multiple_of(me // per * 8, 8), 8)
    both = jnp.concatenate([wts[base, :], wts_t[base, :]], axis=0).astype(BF16)
    parts = jnp.dot(both, emb, preferred_element_type=F32)
    d_emb = LOGIT_SCALE * (parts[:8] + parts[8:])
    unit_own = unit[base, :]
    radial = jnp.sum(d_emb * unit_own, axis=-1, keepdims=True)
    d_proj = ((d_emb - radial * unit_own) * scale[base, :][:, :1]).astype(BF16)
    grad = dot(d_proj, wproj[...], 1, 1)
    part = lax.rem(me, per)
    out = grad[:slots]
    for k in range(1, per):
        out = jnp.where(part == k, grad[k * slots : (k + 1) * slots], out)
    grad_ref[...] = out


def body(n, tokens, seg_ids, counts, positives, w_qkv, w_out, ln_gain, w_proj):
    rows, width = tokens.shape
    slots = positives.shape[0]
    inner = w_out.shape[0]
    embed = w_proj.shape[1]
    block = min(256, rows)
    total = n * slots
    vmem = pl.BlockSpec(memory_space=pltpu.VMEM)
    smem = pl.BlockSpec(memory_space=pltpu.SMEM)
    hbm = pl.BlockSpec(memory_space=pltpu.HBM)
    tokens, seg_hbm, w_qkv, w_out, w_proj = (
        pltpu.with_memory_space_constraint(a, pltpu.HBM)
        for a in (tokens, seg_ids, w_qkv, w_out, w_proj)
    )
    tok, wout, ctx_t = pl.pallas_call(
        functools.partial(attend_kernel, block, slots),
        name="attend",
        out_shape=[
            jax.ShapeDtypeStruct((rows, width), BF16),
            jax.ShapeDtypeStruct(w_out.shape, BF16),
            jax.ShapeDtypeStruct((inner, rows), BF16),
        ],
        in_specs=[hbm, hbm, hbm, hbm],
        out_specs=[vmem, vmem, vmem],
        scratch_shapes=[
            pltpu.VMEM((1, rows), jnp.int32),
            pltpu.VMEM(w_qkv.shape, BF16),
            pltpu.VMEM((inner, rows), BF16),
            pltpu.VMEM((rows, inner), BF16),
            pltpu.VMEM((inner, rows), BF16),
            pltpu.VMEM((rows, 128), BF16),
            pltpu.VMEM((128, rows), BF16),
            pltpu.VMEM((2, rows, block), F32),
            pltpu.SemaphoreType.DMA((rows // block,)),
            pltpu.SemaphoreType.DMA((5,)),
        ],
        compiler_params=pltpu.CompilerParams(vmem_limit_bytes=32 * 1024 * 1024),
    )(seg_hbm, tokens, w_qkv, w_out)
    gath, wproj = pl.pallas_call(
        functools.partial(exchange_kernel, n, slots),
        name="exchange",
        out_shape=[
            jax.ShapeDtypeStruct((n, slots, width + EXT), BF16),
            jax.ShapeDtypeStruct(w_proj.shape, BF16),
        ],
        in_specs=[smem, smem, vmem, vmem, vmem, vmem, vmem, hbm],
        out_specs=[vmem, vmem],
        scratch_shapes=[
            pltpu.VMEM((slots, width + EXT), BF16),
            pltpu.VMEM((8, width), F32),
            pltpu.SemaphoreType.DMA((n // 2,)),
            pltpu.SemaphoreType.DMA((n // 2,)),
            pltpu.SemaphoreType.DMA((n // 2,)),
            pltpu.SemaphoreType.DMA((n // 2,)),
            pltpu.SemaphoreType.DMA,
            pltpu.SemaphoreType.DMA,
        ],
        compiler_params=pltpu.CompilerParams(
            collective_id=0, has_side_effects=True, vmem_limit_bytes=24 * 1024 * 1024
        ),
    )(counts, positives, seg_ids, ln_gain.reshape(1, width), tok, wout, ctx_t, w_proj)
    loss, grad = pl.pallas_call(
        functools.partial(loss_kernel, n, slots),
        name="contrast",
        out_shape=[
            jax.ShapeDtypeStruct((slots,), F32),
            jax.ShapeDtypeStruct((slots, width), F32),
        ],
        in_specs=[vmem, vmem],
        out_specs=[vmem, vmem],
        scratch_shapes=[
            pltpu.VMEM((total, width + EXT), F32),
            pltpu.VMEM((total, embed), F32),
            pltpu.VMEM((total, 128), F32),
            pltpu.VMEM((total, total), F32),
            pltpu.VMEM((total, total), F32),
        ],
        compiler_params=pltpu.CompilerParams(
            vmem_limit_bytes=(24 if total <= 128 else 56) * 1024 * 1024
        ),
    )(gath, wproj)
    return loss, grad


def solution(mesh):
    return jax.shard_map(
        functools.partial(body, mesh.shape["dp"]),
        mesh=mesh,
        in_specs=(P("dp", None), P("dp", None), P(), P("dp"), P(), P(), P(), P()),
        out_specs=(P("dp"), P("dp", None)),
        check_vma=False,
    )
```
